16 devices in a mesh: dp: 2 (over y, z), ep: 8 (over x, core).
Axes of the slice: x: 4, y: 2, z: 1, core: 2. Of those that a mesh axis runs over, the one named last changes fastest.
The devices are a block of a 4x4x8 slice.
Arguments:
- hidden: bfloat16 [2048, 5120], P(('dp', 'ep')), parts along dimension 0
- positions: int32 [2048], P(('dp', 'ep')), parts along dimension 0
- ckv_cache: bfloat16 [2048, 256, 512], P(('dp', 'ep')), parts along dimension 0
- kpe_cache: bfloat16 [2048, 256, 64], P(('dp', 'ep')), parts along dimension 0
- topk_ids: int32 [2048, 6], P(('dp', 'ep')), parts along dimension 0
- attn_gain: bfloat16 [5120], replicated
- w_dq: bfloat16 [5120, 1536], replicated
- q_gain: bfloat16 [1536], replicated
- w_uq: bfloat16 [1536, 3072], replicated
- w_dkv: bfloat16 [5120, 576], replicated
- kv_gain: bfloat16 [512], replicated
- w_uk: bfloat16 [512, 2048], replicated
- w_uv: bfloat16 [512, 2048], replicated
- w_out: bfloat16 [2048, 5120], replicated
- ffn_gain: bfloat16 [5120], replicated
- w_router: bfloat16 [5120, 16], replicated
- w_gate: bfloat16 [16, 5120, 1536], P('ep')
- w_up: bfloat16 [16, 5120, 1536], P('ep')
- w_down: bfloat16 [16, 1536, 5120], P('ep')
- shared_gate: bfloat16 [5120, 3072], replicated
- shared_up: bfloat16 [5120, 3072], replicated
- shared_down: bfloat16 [3072, 5120], replicated
Outputs:
- output 1: bfloat16 [2048, 5120], P(('dp', 'ep')), parts along dimension 0
- output 2: bfloat16 [2048, 512], P(('dp', 'ep')), parts along dimension 0
- output 3: bfloat16 [2048, 64], P(('dp', 'ep')), parts along dimension 0
There are 2 independent parts. The reference program is written for one: setup_inputs(seed, part) draws one part's arguments, and reference() takes and returns one part's arrays. A program takes and returns all parts, laid end to end along the dimension named above; an argument that names none is the same for every part.
All inputs are finite; a program needn't handle non-finite values.
Results may differ from the reference program's by a relative error of at most 0.0153546.
Values are sent between devices in bfloat16 or wider.
A program may use at most 768 MiB of HBM per device.

```python
import jax
import jax.numpy as jnp
from jax import lax

MODEL_DIM = 5120
HEADS = 16
Q_RANK = 1536
KV_RANK = 512
NOPE_DIM = 128
ROPE_DIM = 64
VALUE_DIM = 128
EXPERTS = 16
EXPERT_FF = 1536
SHARED_FF = 3072
TOP_K = 6
N_GROUPS = 8
TOP_GROUPS = 3
TOKENS_DEV = 128
EP_SIZE = 8
CACHE_LEN = 256
CAPACITY = 96

BATCH_PART = EP_SIZE * TOKENS_DEV
QK_DIM = NOPE_DIM + ROPE_DIM
EPSILON = 1e-6
ROUTE_SCALE = 2.5
ROPE_BASE = 10000.0


def draw_routing(key):
    keys = jax.random.split(key, 2)
    rank_of = jax.random.permutation(keys[0], EXPERTS)
    popular = jnp.where(rank_of == 0, 1048576, 4096 // (rank_of + 1))
    noise = jax.random.randint(keys[1], (BATCH_PART, EXPERTS), 0, 4096)
    score = (popular[None, :] + noise) * EXPERTS + jnp.arange(EXPERTS)[None, :]
    group_best = jnp.max(score.reshape(BATCH_PART, N_GROUPS, EXPERTS // N_GROUPS), axis=2)
    group_ids = lax.top_k(group_best, TOP_GROUPS)[1]
    chosen = jnp.any(group_ids[:, :, None] == jnp.arange(N_GROUPS)[None, None, :], axis=1)
    allowed = jnp.repeat(chosen, EXPERTS // N_GROUPS, axis=1)
    masked = jnp.where(allowed, score, -1)
    return lax.top_k(masked, TOP_K)[1].astype(jnp.int32)


def draw_positions(key):
    keys = jax.random.split(key, 2)
    limit = jax.random.randint(keys[0], (EP_SIZE, 1), CACHE_LEN // 8, CACHE_LEN + 1)
    positions = jax.random.randint(keys[1], (EP_SIZE, TOKENS_DEV), 0, limit).reshape(BATCH_PART)
    return positions.at[0].set(CACHE_LEN - 1).astype(jnp.int32)


def draw_normal(key, shape, scale):
    return (jax.random.normal(key, shape, jnp.float32) * scale).astype(jnp.bfloat16)


def draw_gain(key, shape):
    return jax.random.uniform(key, shape, jnp.float32, 0.5, 1.5).astype(jnp.bfloat16)


def draw_stack(key, shape, scale):
    return lax.map(lambda one: draw_normal(one, shape, scale), jax.random.split(key, EXPERTS))


def setup_inputs(seed: int = 0, part: int = 0) -> dict:
    wkeys = jax.random.split(jax.random.key(seed + 1), 18)
    pkeys = jax.random.split(jax.random.fold_in(jax.random.key(seed), part), 6)
    ckv_mean = 0.5 * jax.random.normal(pkeys[2], (BATCH_PART, 1, KV_RANK), jnp.float32)
    ckv_rows = jax.random.normal(pkeys[3], (BATCH_PART, CACHE_LEN, KV_RANK), jnp.float32)
    return {
        'hidden': draw_normal(pkeys[0], (BATCH_PART, MODEL_DIM), 1.0),
        'positions': draw_positions(pkeys[1]),
        'ckv_cache': (ckv_mean + ckv_rows).astype(jnp.bfloat16),
        'kpe_cache': draw_normal(pkeys[4], (BATCH_PART, CACHE_LEN, ROPE_DIM), 1.0),
        'topk_ids': draw_routing(pkeys[5]),
        'attn_gain': draw_gain(wkeys[0], (MODEL_DIM,)),
        'w_dq': draw_normal(wkeys[1], (MODEL_DIM, Q_RANK), MODEL_DIM ** -0.5),
        'q_gain': draw_gain(wkeys[2], (Q_RANK,)),
        'w_uq': draw_normal(wkeys[3], (Q_RANK, HEADS * QK_DIM), Q_RANK ** -0.5),
        'w_dkv': draw_normal(wkeys[4], (MODEL_DIM, KV_RANK + ROPE_DIM), MODEL_DIM ** -0.5),
        'kv_gain': draw_gain(wkeys[5], (KV_RANK,)),
        'w_uk': draw_normal(wkeys[6], (KV_RANK, HEADS * NOPE_DIM), KV_RANK ** -0.5),
        'w_uv': draw_normal(wkeys[7], (KV_RANK, HEADS * VALUE_DIM), KV_RANK ** -0.5),
        'w_out': draw_normal(wkeys[8], (HEADS * VALUE_DIM, MODEL_DIM), (HEADS * VALUE_DIM) ** -0.5),
        'ffn_gain': draw_gain(wkeys[9], (MODEL_DIM,)),
        'w_router': draw_normal(wkeys[10], (MODEL_DIM, EXPERTS), 1.2 * MODEL_DIM ** -0.5),
        'w_gate': draw_stack(wkeys[11], (MODEL_DIM, EXPERT_FF), MODEL_DIM ** -0.5),
        'w_up': draw_stack(wkeys[12], (MODEL_DIM, EXPERT_FF), MODEL_DIM ** -0.5),
        'w_down': draw_stack(wkeys[13], (EXPERT_FF, MODEL_DIM), 2.0 * EXPERT_FF ** -0.5),
        'shared_gate': draw_normal(wkeys[14], (MODEL_DIM, SHARED_FF), MODEL_DIM ** -0.5),
        'shared_up': draw_normal(wkeys[15], (MODEL_DIM, SHARED_FF), MODEL_DIM ** -0.5),
        'shared_down': draw_normal(wkeys[16], (SHARED_FF, MODEL_DIM), 2.0 * SHARED_FF ** -0.5),
    }


def rms_norm(vec, gain):
    vec = vec.astype(jnp.float32)
    scale = lax.rsqrt(jnp.mean(vec * vec, axis=-1, keepdims=True) + EPSILON)
    return vec * scale * gain.astype(jnp.float32)


def rotary(vec, positions):
    half = ROPE_DIM // 2
    freqs = ROPE_BASE ** (-jnp.arange(half).astype(jnp.float32) / half)
    angle = positions.astype(jnp.float32)[..., None] * freqs
    cosine = jnp.cos(angle)
    sine = jnp.sin(angle)
    first = vec[..., :half]
    second = vec[..., half:]
    return jnp.concatenate([first * cosine - second * sine, first * sine + second * cosine], axis=-1)


def attend_one(args):
    q_abs, q_rot, ckv_rows, kpe_rows, c_new, k_new, position = args
    scale = QK_DIM ** -0.5
    s_cache = (jnp.dot(q_abs, ckv_rows.T, preferred_element_type=jnp.float32) + jnp.dot(q_rot, kpe_rows.T, preferred_element_type=jnp.float32)) * scale
    valid = jnp.arange(CACHE_LEN) < position
    s_cache = jnp.where(valid[None, :], s_cache, -1e30)
    s_self = (jnp.dot(q_abs, c_new, preferred_element_type=jnp.float32) + jnp.dot(q_rot, k_new, preferred_element_type=jnp.float32)) * scale
    peak = jnp.maximum(jnp.max(s_cache, axis=1), s_self)
    e_cache = jnp.exp(s_cache - peak[:, None])
    e_self = jnp.exp(s_self - peak)
    denominator = jnp.sum(e_cache, axis=1) + e_self
    p_cache = (e_cache / denominator[:, None]).astype(jnp.bfloat16)
    p_self = (e_self / denominator).astype(jnp.bfloat16)
    context = jnp.dot(p_cache, ckv_rows, preferred_element_type=jnp.float32) + p_self.astype(jnp.float32)[:, None] * c_new.astype(jnp.float32)[None, :]
    return context.astype(jnp.bfloat16)


def expert_apply(args):
    rows, gate_w, up_w, down_w = args
    h_gate = jnp.dot(rows, gate_w, preferred_element_type=jnp.float32)
    h_up = jnp.dot(rows, up_w, preferred_element_type=jnp.float32)
    act = (jax.nn.silu(h_gate) * h_up).astype(jnp.bfloat16)
    return jnp.dot(act, down_w, preferred_element_type=jnp.float32).astype(jnp.bfloat16)


def reference(hidden, positions, ckv_cache, kpe_cache, topk_ids, attn_gain, w_dq, q_gain, w_uq, w_dkv, kv_gain, w_uk, w_uv, w_out, ffn_gain, w_router, w_gate, w_up, w_down, shared_gate, shared_up, shared_down):
    normed = rms_norm(hidden, attn_gain).astype(jnp.bfloat16)
    c_q = rms_norm(jnp.dot(normed, w_dq, preferred_element_type=jnp.float32), q_gain).astype(jnp.bfloat16)
    query = jnp.dot(c_q, w_uq, preferred_element_type=jnp.float32).astype(jnp.bfloat16).reshape(BATCH_PART, HEADS, QK_DIM)
    q_nope = query[:, :, :NOPE_DIM]
    q_rot = rotary(query[:, :, NOPE_DIM:].astype(jnp.float32), positions[:, None]).astype(jnp.bfloat16)
    kv_proj = jnp.dot(normed, w_dkv, preferred_element_type=jnp.float32)
    c_new = rms_norm(kv_proj[:, :KV_RANK], kv_gain).astype(jnp.bfloat16)
    k_new = rotary(kv_proj[:, KV_RANK:], positions).astype(jnp.bfloat16)
    q_abs = jnp.einsum('bhn,chn->bhc', q_nope.astype(jnp.float32), w_uk.reshape(KV_RANK, HEADS, NOPE_DIM).astype(jnp.float32)).astype(jnp.bfloat16)
    context = lax.map(attend_one, (q_abs, q_rot, ckv_cache, kpe_cache, c_new, k_new, positions))
    heads_out = jnp.einsum('bhc,chv->bhv', context.astype(jnp.float32), w_uv.reshape(KV_RANK, HEADS, VALUE_DIM).astype(jnp.float32)).astype(jnp.bfloat16)
    attn_out = jnp.dot(heads_out.reshape(BATCH_PART, HEADS * VALUE_DIM), w_out, preferred_element_type=jnp.float32)
    x_mid = (hidden.astype(jnp.float32) + attn_out).astype(jnp.bfloat16)
    u_norm = rms_norm(x_mid, ffn_gain).astype(jnp.bfloat16)
    gates = jax.nn.sigmoid(jnp.dot(u_norm, w_router, preferred_element_type=jnp.float32))
    chosen = jnp.take_along_axis(gates, topk_ids, axis=1)
    weights = ROUTE_SCALE * chosen / jnp.sum(chosen, axis=1, keepdims=True)
    hits = (topk_ids[:, :, None] == jnp.arange(EXPERTS)[None, None, :]).astype(jnp.int32)
    per_token = jnp.sum(hits, axis=1).reshape(EP_SIZE, TOKENS_DEV, EXPERTS)
    before = (jnp.cumsum(per_token, axis=1) - per_token).reshape(BATCH_PART, EXPERTS)
    rank = jnp.sum(hits * before[:, None, :], axis=2)
    keep = rank < CAPACITY
    source = jnp.arange(BATCH_PART) // TOKENS_DEV
    target_row = jnp.where(keep, topk_ids * (EP_SIZE * CAPACITY) + source[:, None] * CAPACITY + rank, EXPERTS * EP_SIZE * CAPACITY)
    rows_all = jnp.broadcast_to(u_norm[:, None, :], (BATCH_PART, TOP_K, MODEL_DIM)).reshape(BATCH_PART * TOP_K, MODEL_DIM)
    buffer = jnp.zeros((EXPERTS * EP_SIZE * CAPACITY + 1, MODEL_DIM), jnp.bfloat16).at[target_row.reshape(-1)].set(rows_all)
    buffer = buffer[:-1].reshape(EXPERTS, EP_SIZE * CAPACITY, MODEL_DIM)
    results = lax.map(expert_apply, (buffer, w_gate, w_up, w_down)).reshape(EXPERTS * EP_SIZE * CAPACITY, MODEL_DIM)
    results = jnp.concatenate([results, jnp.zeros((1, MODEL_DIM), jnp.bfloat16)], axis=0)
    picked = jnp.take(results, target_row, axis=0).astype(jnp.float32)
    routed = jnp.sum(weights[:, :, None] * picked, axis=1)
    shared_act = (jax.nn.silu(jnp.dot(u_norm, shared_gate, preferred_element_type=jnp.float32)) * jnp.dot(u_norm, shared_up, preferred_element_type=jnp.float32)).astype(jnp.bfloat16)
    shared_out = jnp.dot(shared_act, shared_down, preferred_element_type=jnp.float32).astype(jnp.bfloat16)
    hidden_out = (x_mid.astype(jnp.float32) + routed + shared_out.astype(jnp.float32)).astype(jnp.bfloat16)
    return (hidden_out, c_new, k_new)
```

```python
import functools

import jax
import jax.numpy as jnp
from jax import lax
from jax.experimental import pallas as pl
from jax.experimental.pallas import tpu as pltpu
from jax.sharding import PartitionSpec as P

NOPE_DIM = 128
ROPE_DIM = 64
VALUE_DIM = 128
QK_DIM = NOPE_DIM + ROPE_DIM
EPSILON = 1e-6
ROUTE_SCALE = 2.5
ROPE_BASE = 10000.0
CAP_FACTOR = 2
CORES = 2
F_TILE = 256
D_TILE = 512
MESH = pl.DeviceIdType.MESH


def rms_norm(vec, gain):
    vec = vec.astype(jnp.float32)
    scale = lax.rsqrt(jnp.mean(vec * vec, axis=-1, keepdims=True) + EPSILON)
    return vec * scale * gain.astype(jnp.float32)


def rotary(vec, positions):
    half = ROPE_DIM // 2
    freqs = ROPE_BASE ** (-jnp.arange(half).astype(jnp.float32) / half)
    angle = positions.astype(jnp.float32)[..., None] * freqs
    cosine = jnp.cos(angle)
    sine = jnp.sin(angle)
    first = vec[..., :half]
    second = vec[..., half:]
    return jnp.concatenate([first * cosine - second * sine, first * sine + second * cosine], axis=-1)


def attention_block(hidden, positions, ckv_cache, kpe_cache, attn_gain, w_dq, q_gain, w_uq, w_dkv, kv_gain, w_uk, w_uv, w_out):
    tokens = hidden.shape[0]
    kv_rank = w_uk.shape[0]
    heads = w_uk.shape[1] // NOPE_DIM
    cache_len = ckv_cache.shape[1]
    normed = rms_norm(hidden, attn_gain).astype(jnp.bfloat16)
    c_q = rms_norm(jnp.dot(normed, w_dq, preferred_element_type=jnp.float32), q_gain).astype(jnp.bfloat16)
    query = jnp.dot(c_q, w_uq, preferred_element_type=jnp.float32).astype(jnp.bfloat16).reshape(tokens, heads, QK_DIM)
    q_nope = query[:, :, :NOPE_DIM]
    q_rot = rotary(query[:, :, NOPE_DIM:].astype(jnp.float32), positions[:, None]).astype(jnp.bfloat16)
    kv_proj = jnp.dot(normed, w_dkv, preferred_element_type=jnp.float32)
    c_new = rms_norm(kv_proj[:, :kv_rank], kv_gain).astype(jnp.bfloat16)
    k_new = rotary(kv_proj[:, kv_rank:], positions).astype(jnp.bfloat16)
    q_abs = jnp.einsum('thn,chn->thc', q_nope, w_uk.reshape(kv_rank, heads, NOPE_DIM), preferred_element_type=jnp.float32).astype(jnp.bfloat16)
    scale = QK_DIM ** -0.5
    s_cache = (jnp.einsum('thc,tsc->ths', q_abs, ckv_cache, preferred_element_type=jnp.float32) + jnp.einsum('thr,tsr->ths', q_rot, kpe_cache, preferred_element_type=jnp.float32)) * scale
    valid = jnp.arange(cache_len)[None, None, :] < positions[:, None, None]
    s_cache = jnp.where(valid, s_cache, -1e30)
    s_self = (jnp.einsum('thc,tc->th', q_abs, c_new, preferred_element_type=jnp.float32) + jnp.einsum('thr,tr->th', q_rot, k_new, preferred_element_type=jnp.float32)) * scale
    peak = jnp.maximum(jnp.max(s_cache, axis=2), s_self)
    e_cache = jnp.exp(s_cache - peak[:, :, None])
    e_self = jnp.exp(s_self - peak)
    denominator = jnp.sum(e_cache, axis=2) + e_self
    p_cache = (e_cache / denominator[:, :, None]).astype(jnp.bfloat16)
    p_self = (e_self / denominator).astype(jnp.bfloat16)
    context = jnp.einsum('ths,tsc->thc', p_cache, ckv_cache, preferred_element_type=jnp.float32) + p_self.astype(jnp.float32)[:, :, None] * c_new.astype(jnp.float32)[:, None, :]
    heads_out = jnp.einsum('thc,chv->thv', context.astype(jnp.bfloat16), w_uv.reshape(kv_rank, heads, VALUE_DIM), preferred_element_type=jnp.float32).astype(jnp.bfloat16)
    attn_out = jnp.dot(heads_out.reshape(tokens, heads * VALUE_DIM), w_out, preferred_element_type=jnp.float32)
    x_mid = (hidden.astype(jnp.float32) + attn_out).astype(jnp.bfloat16)
    return x_mid, c_new, k_new


def route_table(u_norm, topk_ids, w_router, local, capacity):
    tokens = u_norm.shape[0]
    experts = w_router.shape[1]
    gates = jax.nn.sigmoid(jnp.dot(u_norm, w_router, preferred_element_type=jnp.float32))
    hits = jnp.any(topk_ids[:, :, None] == jnp.arange(experts), axis=1)
    total = jnp.sum(jnp.where(hits, gates, 0.0), axis=1, keepdims=True)
    group_hits = hits[:, ::local]
    earlier = (jnp.arange(tokens)[:, None] > jnp.arange(tokens)[None, :]).astype(jnp.bfloat16)
    rank = jnp.dot(earlier, group_hits.astype(jnp.bfloat16), preferred_element_type=jnp.float32)
    slots = jnp.where(group_hits & (rank < capacity), rank, -1.0)
    weights = jnp.where(hits, ROUTE_SCALE * gates / total, 0.0)
    table = jnp.concatenate([weights, slots], axis=1).T
    return jnp.pad(table, ((0, -table.shape[0] % 8), (0, 0)))


def moe_kernel(chips, capacity, u_ref, mid_ref, table_ref, gate_ref, up_ref, down_ref, sgate_ref, sup_ref, sdown_ref, out_ref,
               far_u, picked, act, wbuf, eout, agg, stage, landed, one_in, two_plus, two_minus, tables, scales, spread, shared,
               w_sem, table_send, table_recv, u_send, u_recv, pair_send, pair_recv, near_send, one_send, one_recv, two_send, plus_recv, minus_recv, credit):
    tokens, width = u_ref.shape
    local, _, ff = gate_ref.shape
    experts = local * chips * CORES
    half = tokens // 2
    f_blocks = ff // F_TILE
    steps_f = local * f_blocks
    steps_d = width // D_TILE
    cols = D_TILE // F_TILE
    me = lax.axis_index('ep')
    chip = lax.div(me, CORES)
    core = lax.rem(me, CORES)

    def peer(offset, other):
        return lax.rem(chip + offset, chips) * CORES + (1 - core if other else core)

    def remote(src, dst, send_sem, recv_sem, offset, other):
        return pltpu.make_async_remote_copy(src_ref=src, dst_ref=dst, send_sem=send_sem, recv_sem=recv_sem, device_id={'ep': peer(offset, other)}, device_id_type=MESH)

    plus, minus, far = 1, chips - 1, chips // 2
    peers = [(o, q) for q in range(CORES) for o in range(chips) if (o, q) != (0, 0)]

    def u_at(offset, other):
        index = other * chips + offset
        return u_ref if index == 0 else far_u.at[index - 1]

    def expert_in(step, slot):
        e, b = lax.div(step, f_blocks), lax.rem(step, f_blocks)
        at = pl.ds(pl.multiple_of(b * F_TILE, F_TILE), F_TILE)
        return [pltpu.make_async_copy(ref.at[e, :, at], wbuf.at[slot, k], w_sem.at[slot, k]) for k, ref in enumerate((gate_ref, up_ref))]

    def shared_in(step, slot):
        at = pl.ds(pl.multiple_of(step * F_TILE, F_TILE), F_TILE)
        return [pltpu.make_async_copy(ref.at[:, at], wbuf.at[slot, k], w_sem.at[slot, k]) for k, ref in enumerate((sgate_ref, sup_ref))]

    def down_copies(piece, step, slot):
        copies = []
        for e in range(local):
            for h in range(cols):
                at = pl.ds(pl.multiple_of(step * D_TILE + h * F_TILE, F_TILE), F_TILE)
                copies.append(pltpu.make_async_copy(piece(e, at), wbuf.at[slot, e, pl.ds(h * ff, ff)], w_sem.at[slot, e * cols + h]))
        return copies

    def expert_out(step, slot):
        return down_copies(lambda e, at: down_ref.at[e, :, at], step, slot)

    def shared_down(step, slot):
        return down_copies(lambda e, at: sdown_ref.at[pl.ds(e * ff, ff), at], step, slot)

    def begin(copies):
        for copy in copies:
            copy.start()

    def finish(copies):
        for copy in copies:
            copy.wait()

    def stream(step, steps, load, following):
        slot = lax.rem(step, 2)

        @pl.when(step < steps - 1)
        def _():
            begin(load(step + 1, 1 - slot))

        if following is not None:
            @pl.when(step == steps - 1)
            def _():
                begin(following(0, 0))

        finish(load(step, slot))
        return slot

    def gate_up(lhs, load, following):
        rows = lhs.shape[0]

        def body(step, carry):
            slot = stream(step, steps_f, load, following)
            e, b = lax.div(step, f_blocks), lax.rem(step, f_blocks)
            h_gate = jnp.dot(lhs[...], wbuf[slot, 0], preferred_element_type=jnp.float32)
            h_up = jnp.dot(lhs[...], wbuf[slot, 1], preferred_element_type=jnp.float32)
            act[e, pl.ds(0, rows), pl.ds(pl.multiple_of(b * F_TILE, F_TILE), F_TILE)] = (h_gate * jax.nn.sigmoid(h_gate) * h_up).astype(jnp.bfloat16)
            return carry

        lax.fori_loop(0, steps_f, body, 0)

    begin(shared_in(0, 0))
    barrier = pltpu.get_barrier_semaphore()
    for o, q in peers:
        pl.semaphore_signal(barrier, inc=1, device_id={'ep': peer(o, q)}, device_id_type=MESH)
    pl.semaphore_wait(barrier, len(peers))

    def table_copy(k):
        o, q = peers[k]
        back = q * chips + (chips - o) % chips
        return remote(table_ref, tables.at[back], table_send.at[k], table_recv.at[back], o, q)

    for k in range(len(peers)):
        table_copy(k).start()

    top, low = pl.ds(0, half), pl.ds(half, half)
    routes = [
        (u_at(0, 0), u_at(0, 1), 0, 1),
        (u_at(0, 0), u_at(minus, 0), plus, 0),
        (u_at(0, 0), u_at(plus, 0), minus, 0),
        (u_at(minus, 0), u_at(minus, 1), 0, 1),
        (u_at(minus, 0).at[top], u_at(far, 0).at[top], plus, 0),
        (u_at(plus, 0), u_at(plus, 1), 0, 1),
        (u_at(plus, 0).at[low], u_at(far, 0).at[low], minus, 0),
        (u_at(far, 0).at[top], u_at(far, 1).at[top], 0, 1),
        (u_at(far, 0).at[low], u_at(far, 1).at[low], 0, 1),
    ]

    def u_copy(k):
        src, dst, o, q = routes[k]
        return remote(src, dst, u_send.at[k], u_recv.at[k], o, q)

    for k in (1, 2, 0):
        u_copy(k).start()

    gate_up(u_ref, shared_in, shared_down)

    def shared_body(step, carry):
        slot = stream(step, steps_d, shared_down, expert_in)
        for h in range(cols):
            total = None
            for e in range(local):
                piece = jnp.dot(act[e, pl.ds(0, tokens), :], wbuf[slot, e, pl.ds(h * ff, ff), :], preferred_element_type=jnp.float32)
                total = piece if total is None else total + piece
            shared[:, pl.ds(pl.multiple_of(step * D_TILE + h * F_TILE, F_TILE), F_TILE)] = total.astype(jnp.bfloat16)
        return carry

    lax.fori_loop(0, steps_d, shared_body, 0)

    u_copy(1).wait_recv()
    u_copy(4).start()
    u_copy(3).start()
    u_copy(2).wait_recv()
    u_copy(6).start()
    u_copy(5).start()
    for k in range(len(peers)):
        table_copy(k).wait_recv()
    tables[0] = table_ref[...]

    def place_tables(index):
        slot_row = tables[index, pl.ds(experts + me, 1), :]
        slot_col = jnp.transpose(jnp.broadcast_to(slot_row, (tokens, tokens)))
        lane = lax.broadcasted_iota(jnp.int32, (tokens, tokens), 1).astype(jnp.float32)
        spread[index] = jnp.where(slot_col == lane, 1.0, 0.0).astype(jnp.bfloat16)[:, :capacity]
        for e in range(local):
            row = tables[index, pl.ds(me * local + e, 1), :]
            scales[index, e] = jnp.transpose(jnp.broadcast_to(row, (tokens, tokens)))

    def pick(sources):
        for i, (o, q) in enumerate(sources):
            index = q * chips + o
            place_tables(index)
            slot_row = tables[index, pl.ds(experts + me, 1), :]
            line = lax.broadcasted_iota(jnp.int32, (capacity, tokens), 0).astype(jnp.float32)
            place = jnp.where(slot_row == line, 1.0, 0.0).astype(jnp.bfloat16)
            source = u_at(o, q)

            def body(step, carry, i=i, place=place, source=source):
                at = pl.ds(pl.multiple_of(step * D_TILE, D_TILE), D_TILE)
                picked[pl.ds(i * capacity, capacity), at] = jnp.dot(place, source[:, at], preferred_element_type=jnp.float32).astype(jnp.bfloat16)
                return carry

            lax.fori_loop(0, steps_d, body, 0)

    def pair_copy(step):
        slot = lax.rem(step, 2)
        return remote(stage.at[slot], landed.at[step], pair_send.at[slot], pair_recv.at[step], 0, 1)

    def down(sources, offsets, following, pass_on):
        def body(step, carry):
            @pl.when((step >= 1) & (step <= steps_d))
            def _():
                pair_copy(step - 1).start()

            @pl.when(step < steps_d)
            def _():
                slot = stream(step, steps_d, expert_out, following)
                for e in range(local):
                    for h in range(cols):
                        eout[e, :, pl.ds(h * F_TILE, F_TILE)] = jnp.dot(act[e], wbuf[slot, e, pl.ds(h * ff, ff), :], preferred_element_type=jnp.float32).astype(jnp.bfloat16)

                @pl.when(step >= 2)
                def _():
                    pair_copy(step - 2).wait_send()

                for i, (o, q) in enumerate(sources):
                    index = q * chips + o
                    for h in range(cols):
                        at = pl.ds(h * F_TILE, F_TILE)
                        total = None
                        for e in range(local):
                            scale = jnp.concatenate([scales[index, e]] * (F_TILE // tokens), axis=1)
                            piece = jnp.dot(spread[index], eout[e, pl.ds(i * capacity, capacity), at], preferred_element_type=jnp.float32) * scale
                            total = piece if total is None else total + piece
                        if q == 0:
                            agg[o, step, :, at] = total
                        else:
                            stage[slot, offsets.index(o), :, at] = total

            @pl.when((step >= 2) & (step <= steps_d + 1))
            def _():
                block = step - 2
                pair_copy(block).wait_recv()
                for k, o in enumerate(offsets):
                    agg[o, block] = agg[o, block] + landed[block, k]

            @pl.when(step >= 3)
            def _():
                pass_on(step - 3)

            return carry

        lax.fori_loop(0, steps_d + 3, body, 0)
        for step in (steps_d - 2, steps_d - 1):
            pair_copy(step).wait_send()

    def to_plus(src, dst, recv, send, block):
        return remote(src.at[block], dst.at[block], send.at[block], recv.at[block], plus, 0)

    def to_minus(src, dst, recv, send, block):
        return remote(src.at[block], dst.at[block], send.at[block], recv.at[block], minus, 0)

    def even_odd(block, even, odd):
        @pl.when(lax.rem(block, 2) == 0)
        def _():
            even()

        @pl.when(lax.rem(block, 2) == 1)
        def _():
            odd()

    def near_even(block):
        return to_minus(agg.at[minus], two_minus, minus_recv, near_send, block)

    def near_odd(block):
        return to_plus(agg.at[plus], two_plus, plus_recv, near_send, block)

    def far_even(block):
        return to_plus(agg.at[far], one_in, one_recv, one_send, block)

    def far_odd(block):
        return to_minus(agg.at[far], one_in, one_recv, one_send, block)

    def last_even(block):
        return to_plus(agg.at[plus], two_plus, plus_recv, two_send, block)

    def last_odd(block):
        return to_minus(agg.at[minus], two_minus, minus_recv, two_send, block)

    first = (plus, minus)
    u_copy(5).wait_recv()
    u_copy(3).wait_recv()
    pick([(plus, 0), (minus, 0), (plus, 1), (minus, 1)])
    gate_up(picked, expert_in, expert_out)
    u_copy(4).wait_recv()
    u_copy(7).start()
    u_copy(6).wait_recv()
    u_copy(8).start()
    down([(plus, 0), (minus, 0), (plus, 1), (minus, 1)], first, expert_in,
         lambda block: even_odd(block, lambda: near_even(block).start(), lambda: near_odd(block).start()))
    pl.semaphore_signal(credit, inc=1, device_id={'ep': peer(0, 1)}, device_id_type=MESH)

    second = (far, 0)
    for k in (0, 7, 8):
        u_copy(k).wait_recv()
    pick([(far, 0), (0, 0), (far, 1), (0, 1)])
    gate_up(picked, expert_in, expert_out)
    pl.semaphore_wait(credit, 1)
    down([(far, 0), (0, 0), (far, 1), (0, 1)], second, None,
         lambda block: even_odd(block, lambda: far_even(block).start(), lambda: far_odd(block).start()))

    def relay_body(block, carry):
        def even():
            far_even(block).wait_recv()
            agg[plus, block] = agg[plus, block] + one_in[block]
            last_even(block).start()

        def odd():
            far_odd(block).wait_recv()
            agg[minus, block] = agg[minus, block] + one_in[block]
            last_odd(block).start()

        even_odd(block, even, odd)
        return carry

    lax.fori_loop(0, steps_d, relay_body, 0)

    def final_body(block, carry):
        last_even(block).wait_recv()
        last_odd(block).wait_recv()
        at = pl.ds(pl.multiple_of(block * D_TILE, D_TILE), D_TILE)
        routed = agg[0, block] + two_plus[block] + two_minus[block]
        out_ref[:, at] = (mid_ref[:, at].astype(jnp.float32) + routed + shared[:, at].astype(jnp.float32)).astype(jnp.bfloat16)

        def even():
            near_even(block).wait_send()
            far_even(block).wait_send()
            last_even(block).wait_send()

        def odd():
            near_odd(block).wait_send()
            far_odd(block).wait_send()
            last_odd(block).wait_send()

        even_odd(block, even, odd)
        return carry

    lax.fori_loop(0, steps_d, final_body, 0)
    for k in range(len(peers)):
        table_copy(k).wait_send()
    for k in range(len(routes)):
        u_copy(k).wait_send()


def moe_block(u_norm, x_mid, table, w_gate, w_up, w_down, shared_gate, shared_up, shared_down, ep_size, capacity):
    tokens, width = u_norm.shape
    local, _, ff = w_gate.shape
    chips = ep_size // CORES
    blocks = width // D_TILE
    rows = CORES * 2 * capacity
    f32, bf16 = jnp.float32, jnp.bfloat16
    dma = pltpu.SemaphoreType.DMA
    vmem = pl.BlockSpec(memory_space=pltpu.VMEM)
    hbm = pl.BlockSpec(memory_space=pl.ANY)
    return pl.pallas_call(
        functools.partial(moe_kernel, chips, capacity),
        out_shape=jax.ShapeDtypeStruct((tokens, width), bf16),
        in_specs=[vmem] * 3 + [hbm] * 6,
        out_specs=vmem,
        scratch_shapes=[
            pltpu.VMEM((ep_size - 1, tokens, width), bf16),
            pltpu.VMEM((rows, width), bf16),
            pltpu.VMEM((local, rows, ff), bf16),
            pltpu.VMEM((2, local, width, F_TILE), bf16),
            pltpu.VMEM((local, rows, D_TILE), bf16),
            pltpu.VMEM((chips, blocks, tokens, D_TILE), f32),
            pltpu.VMEM((2, 2, tokens, D_TILE), f32),
            pltpu.VMEM((blocks, 2, tokens, D_TILE), f32),
            pltpu.VMEM((blocks, tokens, D_TILE), f32),
            pltpu.VMEM((blocks, tokens, D_TILE), f32),
            pltpu.VMEM((blocks, tokens, D_TILE), f32),
            pltpu.VMEM((ep_size,) + table.shape, f32),
            pltpu.VMEM((ep_size, local, tokens, tokens), f32),
            pltpu.VMEM((ep_size, tokens, capacity), bf16),
            pltpu.VMEM((tokens, width), bf16),
            dma((2, 2 * local)),
            dma((ep_size - 1,)), dma((ep_size,)),
            dma((9,)), dma((9,)),
            dma((2,)), dma((blocks,)),
            dma((blocks,)), dma((blocks,)), dma((blocks,)), dma((blocks,)), dma((blocks,)), dma((blocks,)),
            pltpu.SemaphoreType.REGULAR,
        ],
        compiler_params=pltpu.CompilerParams(collective_id=0, has_side_effects=True, vmem_limit_bytes=67043328),
        name='moe',
    )(u_norm, x_mid, table, w_gate, w_up, w_down, shared_gate, shared_up, shared_down)


def solution(mesh):
    ep_size = mesh.shape['ep']
    batch = P(('dp', 'ep'))
    whole = P()
    by_expert = P('ep')

    def local_step(hidden, positions, ckv_cache, kpe_cache, topk_ids, attn_gain, w_dq, q_gain, w_uq, w_dkv, kv_gain, w_uk, w_uv, w_out, ffn_gain, w_router, w_gate, w_up, w_down, shared_gate, shared_up, shared_down):
        x_mid, c_new, k_new = attention_block(hidden, positions, ckv_cache, kpe_cache, attn_gain, w_dq, q_gain, w_uq, w_dkv, kv_gain, w_uk, w_uv, w_out)
        u_norm = rms_norm(x_mid, ffn_gain).astype(jnp.bfloat16)
        experts = w_router.shape[1]
        capacity = (CAP_FACTOR * topk_ids.size + experts - 1) // experts
        table = route_table(u_norm, topk_ids, w_router, w_gate.shape[0], capacity)
        hidden_out = moe_block(u_norm, x_mid, table, w_gate, w_up, w_down, shared_gate, shared_up, shared_down, ep_size, capacity)
        return hidden_out, c_new, k_new

    in_specs = (batch,) * 5 + (whole,) * 11 + (by_expert,) * 3 + (whole,) * 3
    return jax.shard_map(local_step, mesh=mesh, in_specs=in_specs, out_specs=(batch, batch, batch), check_vma=False)
```

```python
import functools

import jax
import jax.numpy as jnp
from jax import lax
from jax.experimental import pallas as pl
from jax.experimental.pallas import tpu as pltpu
from jax.sharding import PartitionSpec as P

NOPE_DIM = 128
ROPE_DIM = 64
VALUE_DIM = 128
QK_DIM = NOPE_DIM + ROPE_DIM
EPSILON = 1e-6
ROUTE_SCALE = 2.5
ROPE_BASE = 10000.0
CAP_FACTOR = 2
CORES = 2
F_TILE = 256
D_TILE = 512
W_SLOTS = 3
S_SLOTS = 3
P_TILE = 1024
SEQS = 8
PARTS = 2
MESH = pl.DeviceIdType.MESH


def rms_norm(vec, gain):
    vec = vec.astype(jnp.float32)
    scale = lax.rsqrt(jnp.mean(vec * vec, axis=-1, keepdims=True) + EPSILON)
    return vec * scale * gain.astype(jnp.float32)


def rotary(vec, positions):
    half = ROPE_DIM // 2
    freqs = ROPE_BASE ** (-jnp.arange(half).astype(jnp.float32) / half)
    angle = positions.astype(jnp.float32)[..., None] * freqs
    cosine = jnp.cos(angle)
    sine = jnp.sin(angle)
    first = vec[..., :half]
    second = vec[..., half:]
    return jnp.concatenate([first * cosine - second * sine, first * sine + second * cosine], axis=-1)


def attend_kernel(heads, position_ref, q_abs_ref, q_rot_ref, ckv_ref, kpe_ref, c_new_ref, k_new_ref, context_ref, raw):
    _, cache_len, kv_rank = ckv_ref.shape
    f32, bf16 = jnp.float32, jnp.bfloat16
    rows = heads * SEQS
    wide = q_rot_ref.shape[2]
    pair = wide // ROPE_DIM
    scale = QK_DIM ** -0.5

    def per_row(block):
        return jnp.concatenate([block] * heads, axis=0)

    row_seq = lax.broadcasted_iota(jnp.int32, (rows, 1), 0) % SEQS
    for part in range(PARTS):
        seqs = pl.ds(part * SEQS, SEQS)
        q_abs = q_abs_ref[:, seqs, :].reshape(rows, kv_rank)
        q_rot = q_rot_ref[:, seqs, :].reshape(rows, wide)
        ckv = ckv_ref[seqs].reshape(SEQS * cache_len, kv_rank)
        raw[part] = lax.dot_general(ckv, q_abs, (((1,), (1,)), ((), ())), preferred_element_type=f32)
        lane_seq = lax.broadcasted_iota(jnp.int32, (cache_len, rows), 1) % SEQS
        scores = raw[part, pl.ds(0, cache_len)]
        for g in range(1, SEQS):
            scores = jnp.where(lane_seq == g, raw[part, pl.ds(g * cache_len, cache_len)], scores)
        lane_part = lax.broadcasted_iota(jnp.int32, (rows, wide), 1) // ROPE_DIM
        spread = jnp.concatenate([jnp.where(row_seq == g + lane_part, q_rot.astype(f32), 0.0) for g in range(0, SEQS, pair)], axis=1).astype(bf16)
        rope = jnp.dot(spread, kpe_ref[seqs].reshape(SEQS * ROPE_DIM, cache_len), preferred_element_type=f32)
        scores = (scores.T + rope) * scale
        place = lax.broadcasted_iota(jnp.int32, (SEQS, cache_len), 1)
        scores = jnp.where(per_row(place) < per_row(jnp.broadcast_to(position_ref[seqs], (SEQS, cache_len))), scores, -1e30)
        c_new = per_row(c_new_ref[seqs].astype(f32))
        own = jnp.sum(q_abs.astype(f32) * c_new, axis=1, keepdims=True) + jnp.sum(jnp.where(lane_part == 0, q_rot.astype(f32) * per_row(k_new_ref[seqs].astype(f32)), 0.0), axis=1, keepdims=True)
        own = own * scale
        peak = jnp.maximum(jnp.max(scores, axis=1, keepdims=True), own)
        e_cache = jnp.exp(scores - peak)
        e_own = jnp.exp(own - peak)
        denominator = jnp.sum(e_cache, axis=1, keepdims=True) + e_own
        p_cache = e_cache / denominator
        p_own = (e_own / denominator).astype(bf16).astype(f32)
        probs = jnp.concatenate([jnp.where(row_seq == g, p_cache, 0.0).astype(bf16) for g in range(SEQS)], axis=1)
        context = jnp.dot(probs, ckv, preferred_element_type=f32) + p_own * c_new
        context_ref[:, seqs, :] = context.astype(bf16).reshape(heads, SEQS, kv_rank)


def attend(q_abs, q_rot, ckv_cache, kpe_cache, c_new, k_new, positions):
    heads, tokens, kv_rank = q_abs.shape
    cache_len = ckv_cache.shape[1]
    step = SEQS * PARTS
    doubled = jnp.concatenate([q_rot, q_rot], axis=2)
    k_doubled = jnp.concatenate([k_new, k_new], axis=1)
    wide = doubled.shape[2]
    by_head = lambda i: (0, i, 0)
    by_seq = lambda i: (i, 0, 0)
    return pl.pallas_call(
        functools.partial(attend_kernel, heads),
        grid=(tokens // step,),
        out_shape=jax.ShapeDtypeStruct((heads, tokens, kv_rank), jnp.bfloat16),
        in_specs=[
            pl.BlockSpec((step, 1), lambda i: (i, 0)),
            pl.BlockSpec((heads, step, kv_rank), by_head),
            pl.BlockSpec((heads, step, wide), by_head),
            pl.BlockSpec((step, cache_len, kv_rank), by_seq),
            pl.BlockSpec((step, ROPE_DIM, cache_len), by_seq),
            pl.BlockSpec((step, kv_rank), lambda i: (i, 0)),
            pl.BlockSpec((step, wide), lambda i: (i, 0)),
        ],
        out_specs=pl.BlockSpec((heads, step, kv_rank), by_head),
        scratch_shapes=[pltpu.VMEM((PARTS, SEQS * cache_len, heads * SEQS), jnp.float32)],
        compiler_params=pltpu.CompilerParams(dimension_semantics=('arbitrary',), vmem_limit_bytes=40 * 2**20),
        name='attend',
    )(positions[:, None], q_abs, doubled, ckv_cache, jnp.swapaxes(kpe_cache, 1, 2), c_new, k_doubled)


def attention_block(hidden, positions, ckv_cache, kpe_cache, attn_gain, w_dq, q_gain, w_uq, w_dkv, kv_gain, w_uk, w_uv, w_out):
    tokens = hidden.shape[0]
    kv_rank = w_uk.shape[0]
    heads = w_uk.shape[1] // NOPE_DIM
    normed = rms_norm(hidden, attn_gain).astype(jnp.bfloat16)
    c_q = rms_norm(jnp.dot(normed, w_dq, preferred_element_type=jnp.float32), q_gain).astype(jnp.bfloat16)
    query = jnp.dot(c_q, w_uq, preferred_element_type=jnp.float32).astype(jnp.bfloat16).reshape(tokens, heads, QK_DIM)
    q_nope = query[:, :, :NOPE_DIM]
    q_rot = rotary(query[:, :, NOPE_DIM:].astype(jnp.float32), positions[:, None]).astype(jnp.bfloat16)
    kv_proj = jnp.dot(normed, w_dkv, preferred_element_type=jnp.float32)
    c_new = rms_norm(kv_proj[:, :kv_rank], kv_gain).astype(jnp.bfloat16)
    k_new = rotary(kv_proj[:, kv_rank:], positions).astype(jnp.bfloat16)
    q_abs = jnp.einsum('thn,chn->htc', q_nope, w_uk.reshape(kv_rank, heads, NOPE_DIM), preferred_element_type=jnp.float32).astype(jnp.bfloat16)
    context = attend(q_abs, jnp.swapaxes(q_rot, 0, 1), ckv_cache, kpe_cache, c_new, k_new, positions)
    heads_out = jnp.einsum('htc,chv->thv', context, w_uv.reshape(kv_rank, heads, VALUE_DIM), preferred_element_type=jnp.float32).astype(jnp.bfloat16)
    attn_out = jnp.dot(heads_out.reshape(tokens, heads * VALUE_DIM), w_out, preferred_element_type=jnp.float32)
    x_mid = (hidden.astype(jnp.float32) + attn_out).astype(jnp.bfloat16)
    return x_mid, c_new, k_new


def route_table(u_norm, topk_ids, w_router, local, capacity):
    tokens = u_norm.shape[0]
    experts = w_router.shape[1]
    gates = jax.nn.sigmoid(jnp.dot(u_norm, w_router, preferred_element_type=jnp.float32))
    hits = jnp.any(topk_ids[:, :, None] == jnp.arange(experts), axis=1)
    total = jnp.sum(jnp.where(hits, gates, 0.0), axis=1, keepdims=True)
    group_hits = hits[:, ::local]
    earlier = (jnp.arange(tokens)[:, None] > jnp.arange(tokens)[None, :]).astype(jnp.bfloat16)
    rank = jnp.dot(earlier, group_hits.astype(jnp.bfloat16), preferred_element_type=jnp.float32)
    slots = jnp.where(group_hits & (rank < capacity), rank, -1.0)
    weights = jnp.where(hits, ROUTE_SCALE * gates / total, 0.0)
    table = jnp.concatenate([weights, slots], axis=1).T
    return jnp.pad(table, ((0, -table.shape[0] % 8), (0, 0)))


def moe_kernel(chips, capacity, u_ref, mid_ref, table_ref, gate_ref, up_ref, down_ref, sgate_ref, sup_ref, sdown_ref, out_ref,
               far_u, picked, act, sact, wbuf, eout, agg, stage, landed, one_in, two_plus, two_minus, tables, scales, spread,
               w_sem, table_send, table_recv, u_send, u_recv, pair_send, pair_recv, near_send, one_send, one_recv, two_send, plus_recv, minus_recv, credit):
    tokens, width = u_ref.shape
    local, _, ff = gate_ref.shape
    experts = local * chips * CORES
    half = tokens // 2
    f_blocks = ff // F_TILE
    steps_f = local * f_blocks
    steps_d = width // D_TILE
    cols = D_TILE // F_TILE
    me = lax.axis_index('ep')
    chip = lax.div(me, CORES)
    core = lax.rem(me, CORES)

    def peer(offset, other):
        return lax.rem(chip + offset, chips) * CORES + (1 - core if other else core)

    def remote(src, dst, send_sem, recv_sem, offset, other):
        return pltpu.make_async_remote_copy(src_ref=src, dst_ref=dst, send_sem=send_sem, recv_sem=recv_sem, device_id={'ep': peer(offset, other)}, device_id_type=MESH)

    plus, minus, far = 1, chips - 1, chips // 2
    peers = [(o, q) for q in range(CORES) for o in range(chips) if (o, q) != (0, 0)]

    def u_at(offset, other):
        index = other * chips + offset
        return u_ref if index == 0 else far_u.at[index - 1]

    def expert_in(step, slot):
        e, b = lax.div(step, f_blocks), lax.rem(step, f_blocks)
        at = pl.ds(pl.multiple_of(b * F_TILE, F_TILE), F_TILE)
        return [pltpu.make_async_copy(ref.at[e, :, at], wbuf.at[slot, k], w_sem.at[slot, k]) for k, ref in enumerate((gate_ref, up_ref))]

    def shared_in(step, slot):
        at = pl.ds(pl.multiple_of(step * F_TILE, F_TILE), F_TILE)
        return [pltpu.make_async_copy(ref.at[:, at], wbuf.at[slot, k], w_sem.at[slot, k]) for k, ref in enumerate((sgate_ref, sup_ref))]

    def down_copies(piece, step, slot):
        copies = []
        for e in range(local):
            for h in range(cols):
                at = pl.ds(pl.multiple_of(step * D_TILE + h * F_TILE, F_TILE), F_TILE)
                copies.append(pltpu.make_async_copy(piece(e, at), wbuf.at[slot, e, pl.ds(h * ff, ff)], w_sem.at[slot, e * cols + h]))
        return copies

    def expert_out(step, slot):
        return down_copies(lambda e, at: down_ref.at[e, :, at], step, slot)

    def shared_down(step, slot):
        return down_copies(lambda e, at: sdown_ref.at[pl.ds(e * ff, ff), at], step, slot)

    def begin(copies):
        for copy in copies:
            copy.start()

    def finish(copies):
        for copy in copies:
            copy.wait()

    ahead = W_SLOTS - 1

    def start(count, load, base):
        for step in range(count):
            begin(load(step, (base + step) % W_SLOTS))

    def stream(step, high, base, load, following):
        coming = step + ahead
        to = lax.rem(base + coming, W_SLOTS)

        @pl.when(coming < high)
        def _():
            begin(load(coming, to))

        if following is not None:
            @pl.when(coming >= high)
            def _():
                begin(following(coming - high, to))

        slot = lax.rem(base + step, W_SLOTS)
        finish(load(step, slot))
        return slot

    def gate_up(base, lhs, rows, into, load, following, hook):
        def body(step, carry):
            slot = stream(step, steps_f, base, load, following)
            e, b = lax.div(step, f_blocks), lax.rem(step, f_blocks)
            h_gate = jnp.dot(lhs[:rows], wbuf[slot, 0], preferred_element_type=jnp.float32)
            h_up = jnp.dot(lhs[:rows], wbuf[slot, 1], preferred_element_type=jnp.float32)
            into[e, pl.ds(0, rows), pl.ds(pl.multiple_of(b * F_TILE, F_TILE), F_TILE)] = (h_gate * jax.nn.sigmoid(h_gate) * h_up).astype(jnp.bfloat16)
            if hook is not None:
                hook(step)
            return carry

        lax.fori_loop(0, steps_f, body, 0)

    def shared_out(base, low, high, following):
        def body(step, carry):
            slot = stream(step, high, base - low, shared_down, following)
            for h in range(cols):
                total = None
                for e in range(local):
                    piece = jnp.dot(sact[e], wbuf[slot, e, pl.ds(h * ff, ff), :], preferred_element_type=jnp.float32)
                    total = piece if total is None else total + piece
                out_ref[:, pl.ds(pl.multiple_of(step * D_TILE + h * F_TILE, F_TILE), F_TILE)] = total.astype(jnp.bfloat16)
            return carry

        lax.fori_loop(low, high, body, 0)

    with jax.named_scope('enter'):
        start(ahead, shared_in, 0)
        barrier = pltpu.get_barrier_semaphore()
        for o, q in peers:
            pl.semaphore_signal(barrier, inc=1, device_id={'ep': peer(o, q)}, device_id_type=MESH)
        pl.semaphore_wait(barrier, len(peers))

    def table_copy(k):
        o, q = peers[k]
        back = q * chips + (chips - o) % chips
        return remote(table_ref, tables.at[back], table_send.at[k], table_recv.at[back], o, q)

    for k in range(len(peers)):
        table_copy(k).start()

    halves = pl.ds(0, half), pl.ds(half, half)
    routes = {
        'own': (u_at(0, 0), u_at(0, 1), 0, 1),
        'plus0': (u_at(0, 0).at[halves[0]], u_at(minus, 0).at[halves[0]], plus, 0),
        'plus1': (u_at(0, 0).at[halves[1]], u_at(minus, 0).at[halves[1]], plus, 0),
        'minus1': (u_at(0, 0).at[halves[1]], u_at(plus, 0).at[halves[1]], minus, 0),
        'minus0': (u_at(0, 0).at[halves[0]], u_at(plus, 0).at[halves[0]], minus, 0),
        'far0': (u_at(minus, 0).at[halves[0]], u_at(far, 0).at[halves[0]], plus, 0),
        'far1': (u_at(plus, 0).at[halves[1]], u_at(far, 0).at[halves[1]], minus, 0),
    }
    for name, offset in (('plus', minus), ('minus', plus), ('far', far)):
        for h in range(2):
            routes[f'{name}{h}_pair'] = (u_at(offset, 0).at[halves[h]], u_at(offset, 1).at[halves[h]], 0, 1)
    order = list(routes)

    def u_copy(name):
        src, dst, o, q = routes[name]
        k = order.index(name)
        return remote(src, dst, u_send.at[k], u_recv.at[k], o, q)

    def forward(name, *onward):
        u_copy(name).wait_recv()
        for one in onward:
            u_copy(one).start()

    def at_step(step, when, action):
        @pl.when(step == when)
        def _():
            action()

    for name in ('plus0', 'minus1', 'plus1', 'minus0', 'own'):
        u_copy(name).start()

    def first_halves():
        forward('plus0', 'far0', 'plus0_pair')
        forward('minus1', 'far1', 'minus1_pair')

    with jax.named_scope('shared_in'):
        gate_up(0, u_ref, tokens, sact, shared_in, shared_down, lambda step: at_step(step, steps_f * 3 // 4, first_halves))
    early = steps_d // 2
    near_base = steps_f + early
    far_base = near_base + steps_f + steps_d
    own_base = far_base + steps_f + steps_d
    rest_base = own_base + steps_f + steps_d
    with jax.named_scope('shared_out'):
        shared_out(steps_f, 0, early, expert_in)

    def place_tables(index, i):
        slot_row = tables[index, pl.ds(experts + me, 1), :]
        slot_col = jnp.transpose(jnp.broadcast_to(slot_row, (tokens, tokens)))
        lane = lax.broadcasted_iota(jnp.int32, (tokens, tokens), 1).astype(jnp.float32)
        spread[i] = jnp.where(slot_col == lane, 1.0, 0.0).astype(jnp.bfloat16)[:, :capacity]
        for e in range(local):
            row = tables[index, pl.ds(me * local + e, 1), :]
            scales[i, e] = jnp.transpose(jnp.broadcast_to(row, (tokens, tokens)))

    def pick(sources):
        places = []
        for i, (o, q) in enumerate(sources):
            index = q * chips + o
            place_tables(index, i)
            slot_row = tables[index, pl.ds(experts + me, 1), :]
            line = lax.broadcasted_iota(jnp.int32, (capacity, tokens), 0).astype(jnp.float32)
            places.append(jnp.where(slot_row == line, 1.0, 0.0).astype(jnp.bfloat16))

        def body(step, carry):
            at = pl.ds(pl.multiple_of(step * P_TILE, P_TILE), P_TILE)
            for i, (o, q) in enumerate(sources):
                picked[pl.ds(i * capacity, capacity), at] = jnp.dot(places[i], u_at(o, q)[:, at], preferred_element_type=jnp.float32).astype(jnp.bfloat16)
            return carry

        lax.fori_loop(0, width // P_TILE, body, 0)

    def down(base, group, offsets, keep, following, pass_on):
        sources = [(o, q) for q in range(CORES) for o in offsets]
        rows = len(sources) * capacity
        lines = pl.ds(keep, len(offsets))

        def pair_copy(block):
            slot = lax.rem(block, S_SLOTS)
            return remote(stage.at[slot, pl.ds(0, len(offsets))], landed.at[block, lines], pair_send.at[slot], pair_recv.at[group, block], 0, 1)

        def combine(block):
            for i, (o, q) in enumerate(sources):
                total = None
                for e in range(local):
                    scale = jnp.concatenate([scales[i, e]] * (D_TILE // tokens), axis=1)
                    piece = jnp.dot(spread[i], eout[e, pl.ds(i * capacity, capacity), :], preferred_element_type=jnp.float32) * scale
                    total = piece if total is None else total + piece
                if q == 0:
                    agg[o, block] = total
                else:
                    stage[lax.rem(block, S_SLOTS), offsets.index(o)] = total

        def body(step, carry):
            @pl.when((step > S_SLOTS) & (step <= steps_d))
            def _():
                pair_copy(step - 1 - S_SLOTS).wait_send()

            @pl.when(step < steps_d)
            def _():
                slot = stream(step, steps_d, base, expert_out, following)
                combine(jnp.maximum(step - 1, 0))
                for e in range(local):
                    for h in range(cols):
                        eout[e, pl.ds(0, rows), pl.ds(h * F_TILE, F_TILE)] = jnp.dot(act[e, pl.ds(0, rows), :], wbuf[slot, e, pl.ds(h * ff, ff), :], preferred_element_type=jnp.float32).astype(jnp.bfloat16)

            @pl.when(step == steps_d)
            def _():
                combine(step - 1)

            @pl.when((step >= 1) & (step <= steps_d))
            def _():
                pair_copy(step - 1).start()

            if pass_on is not None:
                @pl.when(step >= 4)
                def _():
                    pass_on(step - 4)

            @pl.when((step >= 3) & (step <= steps_d + 2))
            def _():
                block = step - 3
                pair_copy(block).wait_recv()
                for k, o in enumerate(offsets):
                    agg[o, block] = agg[o, block] + landed[block, keep + k]

            return carry

        lax.fori_loop(0, steps_d + (4 if pass_on is not None else 3), body, 0)
        for block in range(steps_d - S_SLOTS, steps_d):
            pair_copy(block).wait_send()

    def to_plus(src, dst, recv, send, block):
        return remote(src.at[block], dst.at[block], send.at[block], recv.at[block], plus, 0)

    def to_minus(src, dst, recv, send, block):
        return remote(src.at[block], dst.at[block], send.at[block], recv.at[block], minus, 0)

    def even_odd(block, even, odd):
        @pl.when(lax.rem(block, 2) == 0)
        def _():
            even()

        @pl.when(lax.rem(block, 2) == 1)
        def _():
            odd()

    def near_even(block):
        return to_minus(agg.at[minus], two_minus, minus_recv, near_send, block)

    def near_odd(block):
        return to_plus(agg.at[plus], two_plus, plus_recv, near_send, block)

    def far_even(block):
        return to_plus(agg.at[far], one_in, one_recv, one_send, block)

    def far_odd(block):
        return to_minus(agg.at[far], one_in, one_recv, one_send, block)

    def last_even(block):
        return to_plus(agg.at[plus], two_plus, plus_recv, two_send, block)

    def last_odd(block):
        return to_minus(agg.at[minus], two_minus, minus_recv, two_send, block)

    with jax.named_scope('rows_in'):
        forward('plus1', 'plus1_pair')
        forward('minus0', 'minus0_pair')
        for k in range(len(peers)):
            table_copy(k).wait_recv()
        tables[0] = table_ref[...]
        for name in ('plus0_pair', 'minus1_pair', 'plus1_pair', 'minus0_pair'):
            u_copy(name).wait_recv()

    def far_halves():
        forward('far0', 'far0_pair')
        forward('far1', 'far1_pair')

    near = (plus, minus)
    with jax.named_scope('pick1'):
        pick([(o, q) for q in range(CORES) for o in near])
    with jax.named_scope('gate_up1'):
        gate_up(near_base, picked, 2 * len(near) * capacity, act, expert_in, expert_out, lambda step: at_step(step, steps_f * 3 // 4, far_halves))
    with jax.named_scope('down1'):
        down(near_base + steps_f, 0, near, 0, expert_in,
             lambda block: even_odd(block, lambda: near_even(block).start(), lambda: near_odd(block).start()))
        pl.semaphore_signal(credit, inc=1, device_id={'ep': peer(0, 1)}, device_id_type=MESH)

    with jax.named_scope('pick2'):
        for name in ('far0_pair', 'far1_pair', 'own'):
            u_copy(name).wait_recv()
        pick([(far, 0), (far, 1)])
    with jax.named_scope('gate_up2'):
        gate_up(far_base, picked, 2 * capacity, act, expert_in, expert_out, None)
        pl.semaphore_wait(credit, 1)
    with jax.named_scope('down2'):
        down(far_base + steps_f, 1, (far,), 0, expert_in,
             lambda block: even_odd(block, lambda: far_even(block).start(), lambda: far_odd(block).start()))

    def relay(block):
        def even():
            far_even(block).wait_recv()
            agg[plus, block] = agg[plus, block] + one_in[block]
            last_even(block).start()

        def odd():
            far_odd(block).wait_recv()
            agg[minus, block] = agg[minus, block] + one_in[block]
            last_odd(block).start()

        even_odd(block, even, odd)

    def relay_late(step):
        @pl.when(step >= steps_f - steps_d)
        def _():
            relay(step - (steps_f - steps_d))

    with jax.named_scope('pick3'):
        pick([(0, 0), (0, 1)])
    with jax.named_scope('gate_up3'):
        gate_up(own_base, picked, 2 * capacity, act, expert_in, expert_out, relay_late)
    with jax.named_scope('down3'):
        down(own_base + steps_f, 2, (0,), 1, lambda step, slot: shared_down(step + early, slot), None)
    with jax.named_scope('shared_rest'):
        shared_out(rest_base, early, steps_d, None)

    def final_body(block, carry):
        last_even(block).wait_recv()
        last_odd(block).wait_recv()
        at = pl.ds(pl.multiple_of(block * D_TILE, D_TILE), D_TILE)
        routed = agg[0, block] + two_plus[block] + two_minus[block]
        out_ref[:, at] = (mid_ref[:, at].astype(jnp.float32) + routed + out_ref[:, at].astype(jnp.float32)).astype(jnp.bfloat16)

        def even():
            near_even(block).wait_send()
            far_even(block).wait_send()
            last_even(block).wait_send()

        def odd():
            near_odd(block).wait_send()
            far_odd(block).wait_send()
            last_odd(block).wait_send()

        even_odd(block, even, odd)
        return carry

    with jax.named_scope('final'):
        lax.fori_loop(0, steps_d, final_body, 0)
        for k in range(len(peers)):
            table_copy(k).wait_send()
        for name in routes:
            u_copy(name).wait_send()


def moe_block(u_norm, x_mid, table, w_gate, w_up, w_down, shared_gate, shared_up, shared_down, ep_size, capacity):
    tokens, width = u_norm.shape
    local, _, ff = w_gate.shape
    chips = ep_size // CORES
    blocks = width // D_TILE
    rows = CORES * 2 * capacity
    f32, bf16 = jnp.float32, jnp.bfloat16
    dma = pltpu.SemaphoreType.DMA
    vmem = pl.BlockSpec(memory_space=pltpu.VMEM)
    hbm = pl.BlockSpec(memory_space=pl.ANY)
    return pl.pallas_call(
        functools.partial(moe_kernel, chips, capacity),
        out_shape=jax.ShapeDtypeStruct((tokens, width), bf16),
        in_specs=[vmem] * 3 + [hbm] * 6,
        out_specs=vmem,
        scratch_shapes=[
            pltpu.VMEM((ep_size - 1, tokens, width), bf16),
            pltpu.VMEM((rows, width), bf16),
            pltpu.VMEM((local, rows, ff), bf16),
            pltpu.VMEM((local, tokens, ff), bf16),
            pltpu.VMEM((W_SLOTS, local, width, F_TILE), bf16),
            pltpu.VMEM((local, rows, D_TILE), bf16),
            pltpu.VMEM((chips, blocks, tokens, D_TILE), f32),
            pltpu.VMEM((S_SLOTS, 2, tokens, D_TILE), f32),
            pltpu.VMEM((blocks, 2, tokens, D_TILE), f32),
            pltpu.VMEM((blocks, tokens, D_TILE), f32),
            pltpu.VMEM((blocks, tokens, D_TILE), f32),
            pltpu.VMEM((blocks, tokens, D_TILE), f32),
            pltpu.VMEM((ep_size,) + table.shape, f32),
            pltpu.VMEM((2 * CORES, local, tokens, tokens), f32),
            pltpu.VMEM((2 * CORES, tokens, capacity), bf16),
            dma((W_SLOTS, 2 * local)),
            dma((ep_size - 1,)), dma((ep_size,)),
            dma((13,)), dma((13,)),
            dma((S_SLOTS,)), dma((3, blocks)),
            dma((blocks,)), dma((blocks,)), dma((blocks,)), dma((blocks,)), dma((blocks,)), dma((blocks,)),
            pltpu.SemaphoreType.REGULAR,
        ],
        compiler_params=pltpu.CompilerParams(collective_id=0, has_side_effects=True, vmem_limit_bytes=67043328),
        name='moe',
    )(u_norm, x_mid, table, w_gate, w_up, w_down, shared_gate, shared_up, shared_down)


def solution(mesh):
    ep_size = mesh.shape['ep']
    batch = P(('dp', 'ep'))
    whole = P()
    by_expert = P('ep')

    def local_step(hidden, positions, ckv_cache, kpe_cache, topk_ids, attn_gain, w_dq, q_gain, w_uq, w_dkv, kv_gain, w_uk, w_uv, w_out, ffn_gain, w_router, w_gate, w_up, w_down, shared_gate, shared_up, shared_down):
        x_mid, c_new, k_new = attention_block(hidden, positions, ckv_cache, kpe_cache, attn_gain, w_dq, q_gain, w_uq, w_dkv, kv_gain, w_uk, w_uv, w_out)
        u_norm = rms_norm(x_mid, ffn_gain).astype(jnp.bfloat16)
        experts = w_router.shape[1]
        capacity = (CAP_FACTOR * topk_ids.size + experts - 1) // experts
        table = route_table(u_norm, topk_ids, w_router, w_gate.shape[0], capacity)
        hidden_out = moe_block(u_norm, x_mid, table, w_gate, w_up, w_down, shared_gate, shared_up, shared_down, ep_size, capacity)
        return hidden_out, c_new, k_new

    in_specs = (batch,) * 5 + (whole,) * 11 + (by_expert,) * 3 + (whole,) * 3
    return jax.shard_map(local_step, mesh=mesh, in_specs=in_specs, out_specs=(batch, batch, batch), check_vma=False)
```

```python
import functools

import jax
import jax.numpy as jnp
from jax import lax
from jax.experimental import pallas as pl
from jax.experimental.pallas import tpu as pltpu
from jax.sharding import PartitionSpec as P

NOPE_DIM = 128
ROPE_DIM = 64
VALUE_DIM = 128
QK_DIM = NOPE_DIM + ROPE_DIM
EPSILON = 1e-6
ROUTE_SCALE = 2.5
ROPE_BASE = 10000.0
CAP_FACTOR = 2
CORES = 2
F_TILE = 256
D_TILE = 512
W_SLOTS = 3
S_SLOTS = 3
P_TILE = 1024
SEQS = 8
HEADS_STEP = 2
PARTS = 2
MESH = pl.DeviceIdType.MESH


def rms_norm(vec, gain):
    vec = vec.astype(jnp.float32)
    scale = lax.rsqrt(jnp.mean(vec * vec, axis=-1, keepdims=True) + EPSILON)
    return vec * scale * gain.astype(jnp.float32)


def rotary(vec, positions):
    half = ROPE_DIM // 2
    freqs = ROPE_BASE ** (-jnp.arange(half).astype(jnp.float32) / half)
    angle = positions.astype(jnp.float32)[..., None] * freqs
    cosine = jnp.cos(angle)
    sine = jnp.sin(angle)
    first = vec[..., :half]
    second = vec[..., half:]
    return jnp.concatenate([first * cosine - second * sine, first * sine + second * cosine], axis=-1)


def attend_kernel(heads, position_ref, q_abs_ref, q_rot_ref, ckv_ref, kpe_ref, c_new_ref, k_new_ref, context_ref, raw):
    _, cache_len, kv_rank = ckv_ref.shape
    f32, bf16 = jnp.float32, jnp.bfloat16
    rows = heads * SEQS
    wide = q_rot_ref.shape[2]
    pair = wide // ROPE_DIM
    scale = QK_DIM ** -0.5

    def per_row(block):
        return jnp.concatenate([block] * heads, axis=0)

    q_all = jnp.concatenate([q_abs_ref[:, pl.ds(part * SEQS, SEQS), :].reshape(rows, kv_rank) for part in range(PARTS)], axis=0)
    everything = lax.dot_general(ckv_ref[...].reshape(PARTS * SEQS * cache_len, kv_rank), q_all, (((1,), (1,)), ((), ())), preferred_element_type=f32)
    for part in range(PARTS):
        raw[part] = everything[part * SEQS * cache_len:(part + 1) * SEQS * cache_len, part * rows:(part + 1) * rows]
    row_seq = lax.broadcasted_iota(jnp.int32, (rows, 1), 0) % SEQS
    for part in range(PARTS):
        seqs = pl.ds(part * SEQS, SEQS)
        q_abs = q_abs_ref[:, seqs, :].reshape(rows, kv_rank)
        q_rot = q_rot_ref[:, seqs, :].reshape(rows, wide)
        ckv = ckv_ref[seqs].reshape(SEQS * cache_len, kv_rank)
        lane_seq = lax.broadcasted_iota(jnp.int32, (cache_len, rows), 1) % SEQS
        scores = raw[part, pl.ds(0, cache_len)]
        for g in range(1, SEQS):
            scores = jnp.where(lane_seq == g, raw[part, pl.ds(g * cache_len, cache_len)], scores)
        lane_part = lax.broadcasted_iota(jnp.int32, (rows, wide), 1) // ROPE_DIM
        spread = jnp.concatenate([jnp.where(row_seq == g + lane_part, q_rot.astype(f32), 0.0) for g in range(0, SEQS, pair)], axis=1).astype(bf16)
        rope = jnp.dot(spread, kpe_ref[seqs].reshape(SEQS * ROPE_DIM, cache_len), preferred_element_type=f32)
        scores = (scores.T + rope) * scale
        place = lax.broadcasted_iota(jnp.int32, (SEQS, cache_len), 1)
        scores = jnp.where(per_row(place) < per_row(jnp.broadcast_to(position_ref[seqs], (SEQS, cache_len))), scores, -1e30)
        c_new = per_row(c_new_ref[seqs].astype(f32))
        own = jnp.sum(q_abs.astype(f32) * c_new, axis=1, keepdims=True) + jnp.sum(jnp.where(lane_part == 0, q_rot.astype(f32) * per_row(k_new_ref[seqs].astype(f32)), 0.0), axis=1, keepdims=True)
        own = own * scale
        peak = jnp.maximum(jnp.max(scores, axis=1, keepdims=True), own)
        e_cache = jnp.exp(scores - peak)
        e_own = jnp.exp(own - peak)
        denominator = jnp.sum(e_cache, axis=1, keepdims=True) + e_own
        p_cache = e_cache / denominator
        p_own = (e_own / denominator).astype(bf16).astype(f32)
        probs = jnp.concatenate([jnp.where(row_seq == g, p_cache, 0.0).astype(bf16) for g in range(SEQS)], axis=1)
        context = jnp.dot(probs, ckv, preferred_element_type=f32) + p_own * c_new
        context_ref[:, seqs, :] = context.astype(bf16).reshape(heads, SEQS, kv_rank)


def attend(q_abs, q_rot, ckv_cache, kpe_cache, c_new, k_new, positions):
    heads, tokens, kv_rank = q_abs.shape
    cache_len = ckv_cache.shape[1]
    step = SEQS * PARTS
    doubled = jnp.concatenate([q_rot, q_rot], axis=2)
    k_doubled = jnp.concatenate([k_new, k_new], axis=1)
    wide = doubled.shape[2]
    by_head = lambda i: (0, i, 0)
    by_seq = lambda i: (i, 0, 0)
    return pl.pallas_call(
        functools.partial(attend_kernel, heads),
        grid=(tokens // step,),
        out_shape=jax.ShapeDtypeStruct((heads, tokens, kv_rank), jnp.bfloat16),
        in_specs=[
            pl.BlockSpec((step, 1), lambda i: (i, 0)),
            pl.BlockSpec((heads, step, kv_rank), by_head),
            pl.BlockSpec((heads, step, wide), by_head),
            pl.BlockSpec((step, cache_len, kv_rank), by_seq),
            pl.BlockSpec((step, ROPE_DIM, cache_len), by_seq),
            pl.BlockSpec((step, kv_rank), lambda i: (i, 0)),
            pl.BlockSpec((step, wide), lambda i: (i, 0)),
        ],
        out_specs=pl.BlockSpec((heads, step, kv_rank), by_head),
        scratch_shapes=[pltpu.VMEM((PARTS, SEQS * cache_len, heads * SEQS), jnp.float32)],
        compiler_params=pltpu.CompilerParams(dimension_semantics=('arbitrary',), vmem_limit_bytes=40 * 2**20),
        name='attend',
    )(positions[:, None], q_abs, doubled, ckv_cache, jnp.swapaxes(kpe_cache, 1, 2), c_new, k_doubled)


def norm_rows(vec, gain):
    return vec * lax.rsqrt(jnp.mean(vec * vec, axis=1, keepdims=True) + EPSILON) * gain.astype(jnp.float32)


def out_proj_kernel(context_ref, uv_ref, out_ref, hidden_ref, gain_ref, mid_ref, u_ref, total):
    step = pl.program_id(0)
    width = hidden_ref.shape[1]

    @pl.when(step == 0)
    def _():
        total[...] = hidden_ref[...].astype(jnp.float32)

    heads = [jnp.dot(context_ref[k], uv_ref[:, k * VALUE_DIM:(k + 1) * VALUE_DIM], preferred_element_type=jnp.float32) for k in range(context_ref.shape[0])]
    heads = jnp.concatenate(heads, axis=1).astype(jnp.bfloat16)
    for c in range(0, width, P_TILE):
        total[:, c:c + P_TILE] += jnp.dot(heads, out_ref[:, c:c + P_TILE], preferred_element_type=jnp.float32)

    @pl.when(step == pl.num_programs(0) - 1)
    def _():
        mid = total[...].astype(jnp.bfloat16)
        mid_ref[...] = mid
        u_ref[...] = norm_rows(mid.astype(jnp.float32), gain_ref[...]).astype(jnp.bfloat16)


def out_proj(context, w_uv, w_out, hidden, ffn_gain):
    heads, tokens, kv_rank = context.shape
    width = hidden.shape[1]
    whole = lambda shape: pl.BlockSpec(shape, lambda i: (0, 0))
    rows = jax.ShapeDtypeStruct((tokens, width), jnp.bfloat16)
    return pl.pallas_call(
        out_proj_kernel,
        grid=(heads // HEADS_STEP,),
        out_shape=(rows, rows),
        in_specs=[
            pl.BlockSpec((HEADS_STEP, tokens, kv_rank), lambda i: (i, 0, 0)),
            pl.BlockSpec((kv_rank, HEADS_STEP * VALUE_DIM), lambda i: (0, i)),
            pl.BlockSpec((HEADS_STEP * VALUE_DIM, width), lambda i: (i, 0)),
            whole((tokens, width)),
            whole((1, width)),
        ],
        out_specs=(whole((tokens, width)), whole((tokens, width))),
        scratch_shapes=[pltpu.VMEM((tokens, width), jnp.float32)],
        compiler_params=pltpu.CompilerParams(dimension_semantics=('arbitrary',), vmem_limit_bytes=32 * 2**20),
        name='out_proj',
    )(context, w_uv, w_out, hidden, ffn_gain[None])


def attention_block(hidden, positions, ckv_cache, kpe_cache, attn_gain, w_dq, q_gain, w_uq, w_dkv, kv_gain, w_uk, w_uv, w_out, ffn_gain):
    tokens = hidden.shape[0]
    kv_rank = w_uk.shape[0]
    heads = w_uk.shape[1] // NOPE_DIM
    normed = rms_norm(hidden, attn_gain).astype(jnp.bfloat16)
    c_q = rms_norm(jnp.dot(normed, w_dq, preferred_element_type=jnp.float32), q_gain).astype(jnp.bfloat16)
    query = jnp.dot(c_q, w_uq, preferred_element_type=jnp.float32).astype(jnp.bfloat16).reshape(tokens, heads, QK_DIM)
    q_nope = query[:, :, :NOPE_DIM]
    q_rot = rotary(query[:, :, NOPE_DIM:].astype(jnp.float32), positions[:, None]).astype(jnp.bfloat16)
    kv_proj = jnp.dot(normed, w_dkv, preferred_element_type=jnp.float32)
    c_new = rms_norm(kv_proj[:, :kv_rank], kv_gain).astype(jnp.bfloat16)
    k_new = rotary(kv_proj[:, kv_rank:], positions).astype(jnp.bfloat16)
    q_abs = jnp.einsum('thn,chn->htc', q_nope, w_uk.reshape(kv_rank, heads, NOPE_DIM), preferred_element_type=jnp.float32).astype(jnp.bfloat16)
    context = attend(q_abs, jnp.swapaxes(q_rot, 0, 1), ckv_cache, kpe_cache, c_new, k_new, positions)
    x_mid, u_norm = out_proj(context, w_uv, w_out, hidden, ffn_gain)
    return x_mid, u_norm, c_new, k_new


def route_table(u_norm, topk_ids, w_router, local, capacity):
    tokens = u_norm.shape[0]
    experts = w_router.shape[1]
    gates = jax.nn.sigmoid(jnp.dot(u_norm, w_router, preferred_element_type=jnp.float32))
    hits = jnp.any(topk_ids[:, :, None] == jnp.arange(experts), axis=1)
    total = jnp.sum(jnp.where(hits, gates, 0.0), axis=1, keepdims=True)
    group_hits = hits[:, ::local]
    earlier = (jnp.arange(tokens)[:, None] > jnp.arange(tokens)[None, :]).astype(jnp.bfloat16)
    rank = jnp.dot(earlier, group_hits.astype(jnp.bfloat16), preferred_element_type=jnp.float32)
    slots = jnp.where(group_hits & (rank < capacity), rank, -1.0)
    weights = jnp.where(hits, ROUTE_SCALE * gates / total, 0.0)
    table = jnp.concatenate([weights, slots], axis=1).T
    return jnp.pad(table, ((0, -table.shape[0] % 8), (0, 0)))


def moe_kernel(chips, capacity, u_ref, mid_ref, table_ref, gate_ref, up_ref, down_ref, sgate_ref, sup_ref, sdown_ref, out_ref,
               far_u, picked, act, sact, wbuf, eout, agg, stage, landed, one_in, two_plus, two_minus, tables, scales, spread,
               w_sem, table_send, table_recv, u_send, u_recv, pair_send, pair_recv, near_send, one_send, one_recv, two_send, plus_recv, minus_recv, mid_sem, credit):
    tokens, width = u_ref.shape
    local, _, ff = gate_ref.shape
    experts = local * chips * CORES
    half = tokens // 2
    f_blocks = ff // F_TILE
    steps_f = local * f_blocks
    steps_d = width // D_TILE
    cols = D_TILE // F_TILE
    me = lax.axis_index('ep')
    chip = lax.div(me, CORES)
    core = lax.rem(me, CORES)

    def peer(offset, other):
        return lax.rem(chip + offset, chips) * CORES + (1 - core if other else core)

    def remote(src, dst, send_sem, recv_sem, offset, other):
        return pltpu.make_async_remote_copy(src_ref=src, dst_ref=dst, send_sem=send_sem, recv_sem=recv_sem, device_id={'ep': peer(offset, other)}, device_id_type=MESH)

    plus, minus, far = 1, chips - 1, chips // 2
    peers = [(o, q) for q in range(CORES) for o in range(chips) if (o, q) != (0, 0)]

    def u_at(offset, other):
        index = other * chips + offset
        return u_ref if index == 0 else far_u.at[index - 1]

    def expert_in(step, slot):
        e, b = lax.div(step, f_blocks), lax.rem(step, f_blocks)
        at = pl.ds(pl.multiple_of(b * F_TILE, F_TILE), F_TILE)
        return [pltpu.make_async_copy(ref.at[e, :, at], wbuf.at[slot, k], w_sem.at[slot, k]) for k, ref in enumerate((gate_ref, up_ref))]

    def shared_in(step, slot):
        at = pl.ds(pl.multiple_of(step * F_TILE, F_TILE), F_TILE)
        return [pltpu.make_async_copy(ref.at[:, at], wbuf.at[slot, k], w_sem.at[slot, k]) for k, ref in enumerate((sgate_ref, sup_ref))]

    def down_copies(piece, step, slot):
        copies = []
        for e in range(local):
            for h in range(cols):
                at = pl.ds(pl.multiple_of(step * D_TILE + h * F_TILE, F_TILE), F_TILE)
                copies.append(pltpu.make_async_copy(piece(e, at), wbuf.at[slot, e, pl.ds(h * ff, ff)], w_sem.at[slot, e * cols + h]))
        return copies

    def expert_out(step, slot):
        return down_copies(lambda e, at: down_ref.at[e, :, at], step, slot)

    def shared_down(step, slot):
        return down_copies(lambda e, at: sdown_ref.at[pl.ds(e * ff, ff), at], step, slot)

    def begin(copies):
        for copy in copies:
            copy.start()

    def finish(copies):
        for copy in copies:
            copy.wait()

    ahead = W_SLOTS - 1

    def start(count, load, base):
        for step in range(count):
            begin(load(step, (base + step) % W_SLOTS))

    def stream(step, high, base, load, following):
        coming = step + ahead
        to = lax.rem(base + coming, W_SLOTS)

        @pl.when(coming < high)
        def _():
            begin(load(coming, to))

        if following is not None:
            @pl.when(coming >= high)
            def _():
                begin(following(coming - high, to))

        slot = lax.rem(base + step, W_SLOTS)
        finish(load(step, slot))
        return slot

    def gate_up(base, lhs, rows, into, places, load, following, hook):
        def body(step, carry):
            slot = stream(step, steps_f, base, load, following)
            e, b = lax.div(step, f_blocks), lax.rem(step, f_blocks)
            h_gate = jnp.dot(lhs[:rows], wbuf[slot, 0], preferred_element_type=jnp.float32)
            h_up = jnp.dot(lhs[:rows], wbuf[slot, 1], preferred_element_type=jnp.float32)
            value = (h_gate * jax.nn.sigmoid(h_gate) * h_up).astype(jnp.bfloat16)
            size = rows // len(places)
            for n, place in enumerate(places):
                into[e, pl.ds(place, size), pl.ds(pl.multiple_of(b * F_TILE, F_TILE), F_TILE)] = value[n * size:(n + 1) * size]
            if hook is not None:
                hook(step)
            return carry

        lax.fori_loop(0, steps_f, body, 0)

    def shared_out(base, following):
        def body(step, carry):
            slot = stream(step, steps_d, base, shared_down, following)
            for h in range(cols):
                total = None
                for e in range(local):
                    piece = jnp.dot(sact[e], wbuf[slot, e, pl.ds(h * ff, ff), :], preferred_element_type=jnp.float32)
                    total = piece if total is None else total + piece
                out_ref[:, pl.ds(pl.multiple_of(step * D_TILE + h * F_TILE, F_TILE), F_TILE)] = total.astype(jnp.bfloat16)
            return carry

        lax.fori_loop(0, steps_d, body, 0)

    with jax.named_scope('enter'):
        start(ahead, shared_in, 0)
        barrier = pltpu.get_barrier_semaphore()
        for o, q in peers:
            pl.semaphore_signal(barrier, inc=1, device_id={'ep': peer(o, q)}, device_id_type=MESH)
        pl.semaphore_wait(barrier, len(peers))

    def table_copy(k):
        o, q = peers[k]
        back = q * chips + (chips - o) % chips
        return remote(table_ref, tables.at[back], table_send.at[k], table_recv.at[back], o, q)

    for k in range(len(peers)):
        table_copy(k).start()

    halves = pl.ds(0, half), pl.ds(half, half)
    routes = {
        'own': (u_at(0, 0), u_at(0, 1), 0, 1),
        'plus0': (u_at(0, 0).at[halves[0]], u_at(minus, 0).at[halves[0]], plus, 0),
        'plus1': (u_at(0, 0).at[halves[1]], u_at(minus, 0).at[halves[1]], plus, 0),
        'minus1': (u_at(0, 0).at[halves[1]], u_at(plus, 0).at[halves[1]], minus, 0),
        'minus0': (u_at(0, 0).at[halves[0]], u_at(plus, 0).at[halves[0]], minus, 0),
        'far0': (u_at(minus, 0).at[halves[0]], u_at(far, 0).at[halves[0]], plus, 0),
        'far1': (u_at(plus, 0).at[halves[1]], u_at(far, 0).at[halves[1]], minus, 0),
    }
    for name, offset in (('plus', minus), ('minus', plus), ('far', far)):
        for h in range(2):
            routes[f'{name}{h}_pair'] = (u_at(offset, 0).at[halves[h]], u_at(offset, 1).at[halves[h]], 0, 1)
    order = list(routes)

    def u_copy(name):
        src, dst, o, q = routes[name]
        k = order.index(name)
        return remote(src, dst, u_send.at[k], u_recv.at[k], o, q)

    def forward(name, *onward):
        u_copy(name).wait_recv()
        for one in onward:
            u_copy(one).start()

    def at_step(step, when, action):
        @pl.when(step == when)
        def _():
            action()

    for name in ('plus0', 'minus1', 'plus1', 'minus0', 'own'):
        u_copy(name).start()

    def first_halves():
        forward('plus0', 'far0', 'plus0_pair')
        forward('minus1', 'far1', 'minus1_pair')

    with jax.named_scope('shared_in'):
        gate_up(0, u_ref, tokens, sact, (0,), shared_in, shared_down, lambda step: at_step(step, steps_f * 3 // 4, first_halves))
    near_base = steps_f + steps_d
    far_base = near_base + steps_f + steps_d
    own_base = far_base + steps_f + steps_d
    with jax.named_scope('shared_out'):
        shared_out(steps_f, expert_in)

    def place_tables(index, i):
        slot_row = tables[index, pl.ds(experts + me, 1), :]
        slot_col = jnp.transpose(jnp.broadcast_to(slot_row, (tokens, tokens)))
        lane = lax.broadcasted_iota(jnp.int32, (tokens, tokens), 1).astype(jnp.float32)
        spread[i] = jnp.where(slot_col == lane, 1.0, 0.0).astype(jnp.bfloat16)[:, :capacity]
        for e in range(local):
            row = tables[index, pl.ds(me * local + e, 1), :]
            scales[i, e] = jnp.transpose(jnp.broadcast_to(row, (tokens, tokens)))

    def pick(sources, kept):
        places = []
        for i, (o, q) in zip(kept, sources):
            index = q * chips + o
            place_tables(index, i)
            slot_row = tables[index, pl.ds(experts + me, 1), :]
            line = lax.broadcasted_iota(jnp.int32, (capacity, tokens), 0).astype(jnp.float32)
            places.append(jnp.where(slot_row == line, 1.0, 0.0).astype(jnp.bfloat16))

        def body(step, carry):
            at = pl.ds(pl.multiple_of(step * P_TILE, P_TILE), P_TILE)
            for i, (o, q) in enumerate(sources):
                picked[pl.ds(i * capacity, capacity), at] = jnp.dot(places[i], u_at(o, q)[:, at], preferred_element_type=jnp.float32).astype(jnp.bfloat16)
            return carry

        lax.fori_loop(0, width // P_TILE, body, 0)

    def down(base, group, chips_in, keep, first, offset, following, pass_on, lag):
        rows = chips_in * CORES * capacity
        lines = pl.ds(keep, chips_in)

        def pair_copy(block):
            slot = lax.rem(block, S_SLOTS)
            return remote(stage.at[slot, pl.ds(0, chips_in)], landed.at[block, lines], pair_send.at[slot], pair_recv.at[group, block], 0, 1)

        def combine(block):
            for k in range(chips_in):
                for q in range(CORES):
                    i = k * CORES + q
                    source = first(block) + i
                    total = None
                    for e in range(local):
                        scale = jnp.concatenate([scales[source, e]] * (D_TILE // tokens), axis=1)
                        piece = jnp.dot(spread[source], eout[e, pl.ds(i * capacity, capacity), :], preferred_element_type=jnp.float32) * scale
                        total = piece if total is None else total + piece
                    if q == 0:
                        agg[offset(block, k), block] = total
                    else:
                        stage[lax.rem(block, S_SLOTS), k] = total

        def body(step, carry):
            if pass_on is not None:
                @pl.when(step > lag)
                def _():
                    pass_on(step - 1 - lag)

            @pl.when((step > S_SLOTS) & (step <= steps_d))
            def _():
                pair_copy(step - 1 - S_SLOTS).wait_send()

            @pl.when(step < steps_d)
            def _():
                slot = stream(step, steps_d, base, expert_out, following)
                combine(jnp.maximum(step - 1, 0))
                lines_in = pl.ds(pl.multiple_of(first(step) * capacity, CORES * capacity), rows)
                for e in range(local):
                    for h in range(cols):
                        eout[e, pl.ds(0, rows), pl.ds(h * F_TILE, F_TILE)] = jnp.dot(act[e, lines_in, :], wbuf[slot, e, pl.ds(h * ff, ff), :], preferred_element_type=jnp.float32).astype(jnp.bfloat16)

            @pl.when(step == steps_d)
            def _():
                combine(step - 1)

            @pl.when((step >= 1) & (step <= steps_d))
            def _():
                pair_copy(step - 1).start()

            @pl.when((step >= lag) & (step < steps_d + lag))
            def _():
                block = step - lag
                pair_copy(block).wait_recv()
                for k in range(chips_in):
                    o = offset(block, k)
                    agg[o, block] = agg[o, block] + landed[block, keep + k]

            return carry

        lax.fori_loop(0, steps_d + lag + (1 if pass_on is not None else 0), body, 0)
        for block in range(steps_d - S_SLOTS, steps_d):
            pair_copy(block).wait_send()

    def to_plus(src, dst, recv, send, block):
        return remote(src.at[block], dst.at[block], send.at[block], recv.at[block], plus, 0)

    def to_minus(src, dst, recv, send, block):
        return remote(src.at[block], dst.at[block], send.at[block], recv.at[block], minus, 0)

    def even_odd(block, even, odd):
        @pl.when(lax.rem(block, 2) == 0)
        def _():
            even()

        @pl.when(lax.rem(block, 2) == 1)
        def _():
            odd()

    def near_even(block):
        return to_minus(agg.at[minus], two_minus, minus_recv, near_send, block)

    def near_odd(block):
        return to_plus(agg.at[plus], two_plus, plus_recv, near_send, block)

    def far_even(block):
        return to_plus(agg.at[far], one_in, one_recv, one_send, block)

    def far_odd(block):
        return to_minus(agg.at[far], one_in, one_recv, one_send, block)

    def last_even(block):
        return to_plus(agg.at[plus], two_plus, plus_recv, two_send, block)

    def last_odd(block):
        return to_minus(agg.at[minus], two_minus, minus_recv, two_send, block)

    with jax.named_scope('rows_in'):
        forward('plus1', 'plus1_pair')
        forward('minus0', 'minus0_pair')
        for k in range(len(peers)):
            table_copy(k).wait_recv()
        tables[0] = table_ref[...]
        for name in ('plus0_pair', 'minus1_pair', 'plus1_pair', 'minus0_pair'):
            u_copy(name).wait_recv()

    def far_halves():
        forward('far0', 'far0_pair')
        forward('far1', 'far1_pair')

    with jax.named_scope('pick1'):
        pick([(plus, 0), (plus, 1), (minus, 0), (minus, 1)], (0, 1, 4, 5))
    with jax.named_scope('gate_up1'):
        gate_up(near_base, picked, 4 * capacity, act, (0, 4 * capacity), expert_in, expert_out, lambda step: at_step(step, steps_f * 3 // 4, far_halves))
    with jax.named_scope('down1'):
        down(near_base + steps_f, 0, 1, 1, lambda block: (1 - lax.rem(block, 2)) * 2 * CORES, lambda block, k: plus + (1 - lax.rem(block, 2)) * (minus - plus), expert_in,
             lambda block: even_odd(block, lambda: near_even(block).start(), lambda: near_odd(block).start()), 3)
        pl.semaphore_signal(credit, inc=1, device_id={'ep': peer(0, 1)}, device_id_type=MESH)

    with jax.named_scope('pick2'):
        for name in ('far0_pair', 'far1_pair', 'own'):
            u_copy(name).wait_recv()
        pick([(far, 0), (far, 1)], (2, 3))
    with jax.named_scope('gate_up2'):
        gate_up(far_base, picked, 2 * capacity, act, (2 * capacity,), expert_in, expert_out, None)
        pl.semaphore_wait(credit, 1)
    with jax.named_scope('down2'):
        down(far_base + steps_f, 1, 2, 0, lambda block: lax.rem(block, 2) * CORES, lambda block, k: plus + lax.rem(block, 2) + k, expert_in,
             lambda block: even_odd(block, lambda: far_even(block).start(), lambda: far_odd(block).start()), 2)

    def relay(block):
        def even():
            far_even(block).wait_recv()
            agg[plus, block] = agg[plus, block] + one_in[block]
            last_even(block).start()

        def odd():
            far_odd(block).wait_recv()
            agg[minus, block] = agg[minus, block] + one_in[block]
            last_odd(block).start()

        even_odd(block, even, odd)

    def relay_late(step):
        @pl.when(step >= steps_f - steps_d)
        def _():
            relay(step - (steps_f - steps_d))

    pl.semaphore_signal(credit, inc=1, device_id={'ep': peer(0, 1)}, device_id_type=MESH)
    with jax.named_scope('pick3'):
        pick([(0, 0), (0, 1)], (0, 1))
    with jax.named_scope('gate_up3'):
        gate_up(own_base, picked, 2 * capacity, act, (0,), expert_in, expert_out, relay_late)
    late_mid = u_at(far, 1)
    mid_copy = pltpu.make_async_copy(mid_ref, late_mid, mid_sem)
    mid_copy.start()
    with jax.named_scope('down3'):
        pl.semaphore_wait(credit, 1)
        down(own_base + steps_f, 2, 1, 0, lambda block: 0, lambda block, k: 0, None, None, 3)

    def final_body(block, carry):
        last_even(block).wait_recv()
        last_odd(block).wait_recv()
        at = pl.ds(pl.multiple_of(block * D_TILE, D_TILE), D_TILE)
        routed = agg[0, block] + two_plus[block] + two_minus[block]
        out_ref[:, at] = (late_mid[:, at].astype(jnp.float32) + routed + out_ref[:, at].astype(jnp.float32)).astype(jnp.bfloat16)

        def even():
            near_even(block).wait_send()
            far_even(block).wait_send()
            last_even(block).wait_send()

        def odd():
            near_odd(block).wait_send()
            far_odd(block).wait_send()
            last_odd(block).wait_send()

        even_odd(block, even, odd)
        return carry

    with jax.named_scope('final'):
        mid_copy.wait()
        lax.fori_loop(0, steps_d, final_body, 0)
        for k in range(len(peers)):
            table_copy(k).wait_send()
        for name in routes:
            u_copy(name).wait_send()


def moe_block(u_norm, x_mid, table, w_gate, w_up, w_down, shared_gate, shared_up, shared_down, ep_size, capacity):
    tokens, width = u_norm.shape
    local, _, ff = w_gate.shape
    chips = ep_size // CORES
    blocks = width // D_TILE
    rows = CORES * 2 * capacity
    f32, bf16 = jnp.float32, jnp.bfloat16
    dma = pltpu.SemaphoreType.DMA
    vmem = pl.BlockSpec(memory_space=pltpu.VMEM)
    hbm = pl.BlockSpec(memory_space=pl.ANY)
    return pl.pallas_call(
        functools.partial(moe_kernel, chips, capacity),
        out_shape=jax.ShapeDtypeStruct((tokens, width), bf16),
        in_specs=[vmem, hbm, vmem] + [hbm] * 6,
        out_specs=vmem,
        scratch_shapes=[
            pltpu.VMEM((ep_size - 1, tokens, width), bf16),
            pltpu.VMEM((rows, width), bf16),
            pltpu.VMEM((local, 3 * CORES * capacity, ff), bf16),
            pltpu.VMEM((local, tokens, ff), bf16),
            pltpu.VMEM((W_SLOTS, local, width, F_TILE), bf16),
            pltpu.VMEM((local, rows, D_TILE), bf16),
            pltpu.VMEM((chips, blocks, tokens, D_TILE), f32),
            pltpu.VMEM((S_SLOTS, 2, tokens, D_TILE), f32),
            pltpu.VMEM((blocks, 2, tokens, D_TILE), f32),
            pltpu.VMEM((blocks, tokens, D_TILE), f32),
            pltpu.VMEM((blocks, tokens, D_TILE), f32),
            pltpu.VMEM((blocks, tokens, D_TILE), f32),
            pltpu.VMEM((ep_size,) + table.shape, f32),
            pltpu.VMEM((3 * CORES, local, tokens, tokens), f32),
            pltpu.VMEM((3 * CORES, tokens, capacity), bf16),
            dma((W_SLOTS, 2 * local)),
            dma((ep_size - 1,)), dma((ep_size,)),
            dma((13,)), dma((13,)),
            dma((S_SLOTS,)), dma((3, blocks)),
            dma((blocks,)), dma((blocks,)), dma((blocks,)), dma((blocks,)), dma((blocks,)), dma((blocks,)),
            dma(()), pltpu.SemaphoreType.REGULAR,
        ],
        compiler_params=pltpu.CompilerParams(collective_id=0, has_side_effects=True, vmem_limit_bytes=67043328),
        name='moe',
    )(u_norm, x_mid, table, w_gate, w_up, w_down, shared_gate, shared_up, shared_down)


def solution(mesh):
    ep_size = mesh.shape['ep']
    batch = P(('dp', 'ep'))
    whole = P()
    by_expert = P('ep')

    def local_step(hidden, positions, ckv_cache, kpe_cache, topk_ids, attn_gain, w_dq, q_gain, w_uq, w_dkv, kv_gain, w_uk, w_uv, w_out, ffn_gain, w_router, w_gate, w_up, w_down, shared_gate, shared_up, shared_down):
        x_mid, u_norm, c_new, k_new = attention_block(hidden, positions, ckv_cache, kpe_cache, attn_gain, w_dq, q_gain, w_uq, w_dkv, kv_gain, w_uk, w_uv, w_out, ffn_gain)
        experts = w_router.shape[1]
        capacity = (CAP_FACTOR * topk_ids.size + experts - 1) // experts
        table = route_table(u_norm, topk_ids, w_router, w_gate.shape[0], capacity)
        hidden_out = moe_block(u_norm, x_mid, table, w_gate, w_up, w_down, shared_gate, shared_up, shared_down, ep_size, capacity)
        return hidden_out, c_new, k_new

    in_specs = (batch,) * 5 + (whole,) * 11 + (by_expert,) * 3 + (whole,) * 3
    return jax.shard_map(local_step, mesh=mesh, in_specs=in_specs, out_specs=(batch, batch, batch), check_vma=False)
```
